256 devices in a mesh: groups: 4 (over y, x), feat: 64 (over z, core).
Axes of the slice: x: 2, y: 2, z: 32, core: 2. Of those that a mesh axis runs over, the one named last changes fastest.
The devices are a block of a 4x8x32 slice.
Arguments:
- design: float32 [2048, 131072], P('groups', 'feat'), parts along dimension 0, may hold values from -6 to 6
- targets: float32 [2048, 128], P('groups'), parts along dimension 0, may hold values from -6 to 6
- coef_now: float32 [524288, 128], P(('groups', 'feat')), parts along dimension 0, may hold values from -1 to 1
- coef_prev: float32 [524288, 128], P(('groups', 'feat')), parts along dimension 0, may hold values from -1 to 1
- penalty: float32 [512], P('groups'), parts along dimension 0, may hold values from 0.1 to 1
- drop_mask: int32 [4096], P(('groups', 'feat')), parts along dimension 0, may hold values from 0 to 1, as said below
- dest_shard: int32 [4096], P(('groups', 'feat')), parts along dimension 0, may hold values from 0 to 63, as said below
Outputs:
- coef_out: float32 [786432, 128], P(('groups', 'feat')), parts along dimension 0
- design_out: float32 [2048, 196608], P('groups', 'feat'), parts along dimension 0
- duality_gap: float32 [512], P('groups'), parts along dimension 0
- dual_value: float32 [512], P('groups'), parts along dimension 0
- coef_l1: float32 [512], P('groups'), parts along dimension 0
The draws below stay inside these ranges and needn't reach their ends.
There are 4 independent parts, one for each index of `groups`. The reference program is written for one: setup_inputs(seed, part) draws one part's arguments, and reference() takes and returns one part's arrays. A program takes and returns all parts, laid end to end along the dimension named above; each array names one. Nothing has to cross between parts.
Inputs may be any that keep to these rules, and one draw needn't show every extreme that they name: `drop_mask`: screening marks blocks to drop with 1; shards drop very different shares of their blocks. `dest_shard`: a block's destination is its own shard, except that any of the first 4 blocks of a shard may go to the shard before it (cyclically) and any of the last 4 blocks to the shard after it; no shard receives more than 24 surviving blocks, and some shard receives exactly 24 in every draw.
All inputs are finite; a program needn't handle non-finite values.
Results may differ from the reference program's by a relative error of at most 0.0003.
Values sent between devices are 32-bit elements; how exact they have to be, the bound alone decides.
A program may use at most 64 MiB of HBM per device.

```python
import math
import jax
import jax.numpy as jnp
from jax import lax

NSAMP = 512
PHENO = 128
START = 40
BLK_DEV = 16
EDGE = 4
SLOTS = 24
FEATURES = 131072
NBLOCKS = 1024


def block_layout(key):
    shards = NBLOCKS // BLK_DEV
    base = jax.random.fold_in(key, 9137)
    key_star, key_level, key_rolled, key_sideways = jax.random.split(base, 4)
    star = jax.random.randint(key_star, (), 0, shards)
    levels = jax.random.randint(key_level, (shards, 1), 0, 4)
    rolled = jax.random.randint(key_rolled, (shards, BLK_DEV), 0, 8)
    sideways = jax.random.randint(key_sideways, (shards, BLK_DEV), 0, 2)
    position = jnp.arange(BLK_DEV)[None, :]
    owners = jnp.arange(shards)[:, None]
    dropped = rolled < 2 * levels
    offsets = jnp.where(position < EDGE, -sideways, jnp.where(position >= BLK_DEV - EDGE, sideways, 0))
    at_star = owners == star
    before_star = (owners == (star + shards - 1) % shards) & (position >= BLK_DEV - EDGE)
    after_star = (owners == (star + 1) % shards) & (position < EDGE)
    forced = at_star | before_star | after_star
    dropped = jnp.where(forced, False, dropped)
    offsets = jnp.where(at_star, 0, jnp.where(before_star, 1, jnp.where(after_star, -1, offsets)))
    targets_of = (owners + offsets + shards) % shards
    return (dropped.astype(jnp.int32).reshape(-1), targets_of.astype(jnp.int32).reshape(-1))


def draw_drop_mask(key, part):
    return block_layout(key)[0]


def draw_dest_shard(key, part):
    return block_layout(key)[1]


def sparse_coefficients(key, which):
    support_key = jax.random.fold_in(key, 4411)
    keep = jax.random.bernoulli(support_key, 0.01, (FEATURES, PHENO))
    value_key = jax.random.fold_in(key, which)
    position = jnp.arange(FEATURES, dtype=jnp.float32)[:, None] / FEATURES
    rise = 1.0 + 3.0 * position
    values = jnp.clip(jax.random.normal(value_key, (FEATURES, PHENO), jnp.float32), -4.0, 4.0)
    return jnp.where(keep, 0.02 * rise * values, 0.0).astype(jnp.float32)


def draw_coef_now(key, part):
    return sparse_coefficients(key, 731)


def draw_coef_prev(key, part):
    return sparse_coefficients(key, 857)


def block_levels(rng, shape, pieces, least, largest):
    loudness = 1.0
    for dim, parts in pieces:
        heights = jax.random.uniform(jax.random.fold_in(jax.random.fold_in(rng, 6), dim), (parts,), jnp.float32, least / len(pieces), largest / len(pieces))
        loudness = loudness * jnp.repeat(jnp.exp(heights), shape[dim] // parts).reshape((-1,) + (1,) * (len(shape) - 1 - dim))
    return loudness


def scatter_about(rng, extent, width, reach, cuts=(), kind=jnp.bfloat16):
    entries = jax.random.normal(rng, extent, jnp.float32) * width
    if len(cuts) > 0:
        entries = block_levels(rng, extent, cuts, -0.22, 0.18) * entries
    return jnp.clip(entries, min=-reach, max=reach).astype(kind)


def setup_inputs(seed: int = 0, part: int = 0) -> dict:
    keys = jax.random.split(jax.random.key(seed), 8)
    part_splits = jax.random.split(jax.random.fold_in(keys[7], part), 8)
    design = scatter_about(part_splits[0], (NSAMP, FEATURES), 1.0, 6.0, ((1, 64),), jnp.float32)
    targets = scatter_about(part_splits[1], (NSAMP, PHENO), 1.0, 6.0, (), jnp.float32)
    coef_now = draw_coef_now(jax.random.fold_in(jax.random.fold_in(keys[7], part), 71), part)
    coef_prev = draw_coef_prev(jax.random.fold_in(jax.random.fold_in(keys[7], part), 71), part)
    penalty = jnp.clip(jnp.exp(jax.random.uniform(part_splits[4], (PHENO,), jnp.float32, math.log(0.1), math.log(1.0))), 0.1, 1.0)
    drop_mask = draw_drop_mask(jax.random.fold_in(jax.random.fold_in(keys[7], part), 71), part)
    dest_shard = draw_dest_shard(jax.random.fold_in(jax.random.fold_in(keys[7], part), 71), part)
    return {"design": design, "targets": targets, "coef_now": coef_now, "coef_prev": coef_prev, "penalty": penalty, "drop_mask": drop_mask, "dest_shard": dest_shard}


precise = lax.Precision.HIGHEST

def shrink(values, level):
    return jnp.sign(values) * jnp.maximum(jnp.abs(values) - level, 0.0)

def reference(design, targets, coef_now, coef_prev, penalty, drop_mask, dest_shard):
    lipschitz = (math.sqrt(NSAMP) + math.sqrt(FEATURES)) ** 2
    level = penalty * (NSAMP / lipschitz)
    first_push = (START - 1) / (START + 2)
    second_push = START / (START + 3)

    def fitted(point):
        return jnp.dot(design, point, precision=precise, preferred_element_type=jnp.float32)

    def correlate(misfit):
        return lax.dot_general(design, misfit, (((0,), (0,)), ((), ())), precision=precise, preferred_element_type=jnp.float32)

    def descend(point):
        misfit = fitted(point) - targets
        return shrink(point - correlate(misfit) / lipschitz, level)
    coef_one = descend(coef_now + first_push * (coef_now - coef_prev))
    coef_two = descend(coef_one + second_push * (coef_one - coef_now))
    residual = targets - fitted(coef_two)
    correlation = correlate(residual)
    peak = lax.optimization_barrier(jnp.max(jnp.abs(correlation), axis=0))
    coef_l1 = lax.optimization_barrier(jnp.sum(jnp.abs(coef_two), axis=0))
    dual_scale = jnp.maximum(penalty, peak / NSAMP)
    dual_point = targets - penalty * residual / dual_scale
    dual_value = (lax.optimization_barrier(jnp.sum(targets * targets, axis=0)) - lax.optimization_barrier(jnp.sum(dual_point * dual_point, axis=0))) / (2.0 * NSAMP)
    primal = lax.optimization_barrier(jnp.sum(residual * residual, axis=0)) / (2.0 * NSAMP) + penalty * coef_l1
    duality_gap = primal - dual_value
    shards = NBLOCKS // BLK_DEV
    design_blocks = design.reshape(NSAMP, shards, BLK_DEV, 128)
    coef_blocks = coef_two.reshape(shards, BLK_DEV, 128, PHENO)
    survive = (drop_mask == 0).reshape(shards, BLK_DEV)
    destination = dest_shard.reshape(shards, BLK_DEV)
    owners = jnp.arange(shards, dtype=jnp.int32)[:, None]
    staying = survive & (destination == owners)
    to_right = survive & (destination == (owners + 1) % shards)
    to_left = survive & (destination == (owners + shards - 1) % shards)
    arrived = jnp.concatenate([jnp.roll(to_right, 1, axis=0)[:, BLK_DEV - EDGE:], staying, jnp.roll(to_left, -1, axis=0)[:, :EDGE]], axis=1).astype(jnp.int32)
    slot_of = jnp.cumsum(arrived, axis=1, dtype=jnp.int32) - 1
    placement = ((slot_of[:, :, None] == jnp.arange(SLOTS, dtype=jnp.int32)[None, None, :]) & (arrived[:, :, None] > 0)).astype(jnp.float32)
    design_cands = jnp.concatenate([jnp.roll(design_blocks, 1, axis=1)[:, :, BLK_DEV - EDGE:], design_blocks, jnp.roll(design_blocks, -1, axis=1)[:, :, :EDGE]], axis=2)
    design_out = jnp.einsum('nscf,scj->nsjf', design_cands, placement, precision=precise).reshape(NSAMP, shards * SLOTS * 128)
    coef_cands = jnp.concatenate([jnp.roll(coef_blocks, 1, axis=0)[:, BLK_DEV - EDGE:], coef_blocks, jnp.roll(coef_blocks, -1, axis=0)[:, :EDGE]], axis=1)
    coef_out = jnp.einsum('scfk,scj->sjfk', coef_cands, placement, precision=precise).reshape(shards * SLOTS * 128, PHENO)
    return (coef_out, design_out, duality_gap, dual_value, coef_l1)
```

```python
import functools
import math

import jax
import jax.numpy as jnp
from jax import lax
from jax.experimental import pallas as pl
from jax.experimental.pallas import tpu as pltpu
from jax.sharding import PartitionSpec as P

START = 40
NEAR = 8
REACH = NEAR // 2
BLOCK = 128
CHUNKS = 4
MESH = pl.DeviceIdType.MESH
f32 = jnp.float32
bf16 = jnp.bfloat16


def at(device):
    return {"feat": device}


def halves(value):
    high = value.astype(bf16)
    return high, (value - high.astype(f32)).astype(bf16)


def fit_kernel(
    design, targets, now, prev, penalty, drop, dest,
    coef_home, edge_design, edge_coef, flags, stats,
    coef_two, raw, tgt, cur, old, pen, drop_in, dest_in, rows, cols, wide, point, corr,
    part, half, sent, near, own, far, total, misfit, mine, theirs, both, fin,
    load_sem, pair_send, pair_recv, near_send, near_recv, far_send, far_recv,
    all_send, all_recv, pass_send, pass_recv, edge_send, edge_recv, end_send, end_recv, word,
):
    samples, feats = raw.shape
    half_rows = samples // 2
    piece = half_rows // NEAR
    chunk = feats // CHUNKS
    devices = lax.axis_size("feat")
    chips = devices // 2
    blocks = chips // NEAR
    lipschitz = (math.sqrt(samples) + math.sqrt(feats * devices)) ** 2
    first_push = (START - 1) / (START + 2)
    second_push = START / (START + 3)
    edge = feats // 4
    me = lax.axis_index("feat")
    z = me // 2
    c = lax.rem(me, 2)
    partner = z * 2 + 1 - c
    after = lax.rem(me + 1, devices)
    before = lax.rem(me + devices - 1, devices)
    k = lax.rem(z, NEAR)
    block = z // NEAR

    def chip(d):
        return lax.rem(z + d + chips, chips)

    def same(d):
        return chip(d) * 2 + c

    barrier = pltpu.get_barrier_semaphore()

    def hello(semaphore, device):
        pl.semaphore_signal(semaphore, inc=1, device_id=at(device), device_id_type=MESH)

    for d in range(1, REACH + 1):
        hello(barrier, same(d))
        hello(barrier, same(-d))
    hello(barrier, before)
    hello(barrier, after)

    loads = [
        pltpu.make_async_copy(now, cur, load_sem.at[0]),
        pltpu.make_async_copy(prev, old, load_sem.at[1]),
    ]
    for i in range(CHUNKS):
        part_of = pl.ds(i * chunk, chunk)
        loads.append(pltpu.make_async_copy(design.at[:, part_of], raw.at[:, part_of], load_sem.at[2 + i]))
    for i, (source, target) in enumerate(((targets, tgt), (penalty, pen), (drop, drop_in), (dest, dest_in))):
        loads.append(pltpu.make_async_copy(source, target, load_sem.at[2 + CHUNKS + i]))
    for load in loads:
        load.start()

    def remote(source, target, send, recv, device):
        return pltpu.make_async_remote_copy(
            src_ref=source, dst_ref=target, send_sem=send, recv_sem=recv, device_id=at(device), device_id_type=MESH
        )

    def drain(ref, sem):
        pltpu.make_async_copy(ref, ref, sem).wait()

    def set_point(i, value):
        high, low = halves(value)
        here = pl.ds(i * chunk, chunk)
        wide[here, 0:BLOCK] = high
        wide[here, BLOCK : 2 * BLOCK] = low
        point[here, :] = value

    def fitted(h):
        both_parts = jnp.dot(rows[h], wide[...], preferred_element_type=f32)
        summed = both_parts[:half_rows] + both_parts[half_rows:]
        return summed[:, :BLOCK] + summed[:, BLOCK:]

    loads[0].wait()
    loads[1].wait()
    for i in range(CHUNKS):
        here = pl.ds(i * chunk, chunk)
        set_point(i, cur[here, :] + first_push * (cur[here, :] - old[here, :]))
    for i in range(CHUNKS):
        loads[2 + i].wait()
        here = pl.ds(i * chunk, chunk)
        for h in range(2):
            high, low = halves(raw[h * half_rows : (h + 1) * half_rows, here])
            rows[h, 0:half_rows, here] = high
            rows[h, half_rows : 2 * half_rows, here] = low
    for load in loads[2 + CHUNKS :]:
        load.wait()
    level = pen[...] * (samples / lipschitz)
    flags[0:8, :] = jnp.zeros((8, BLOCK), jnp.int32)
    flags[0:1, 0 : drop_in.shape[1]] = drop_in[...]
    flags[1:2, 0 : dest_in.shape[1]] = dest_in[...]

    def transpose_design():
        for h in range(2):
            for p in range(2):
                for i in range(CHUNKS):
                    tile = rows[h, p * half_rows : (p + 1) * half_rows, i * chunk : (i + 1) * chunk]
                    cols[h, i, p * chunk : (p + 1) * chunk, :] = tile.T

    def design_edges(h):
        some = pl.ds(h * half_rows, half_rows)
        return [
            remote(
                design.at[some, pl.ds(first, edge)], edge_design.at[side, some],
                edge_send.at[2 * h + side], edge_recv.at[2 * h + side], device,
            )
            for side, first, device in ((0, feats - edge, after), (1, 0, before))
        ]

    edges = (
        design_edges(0)
        + design_edges(1)
        + [
            remote(coef_two.at[pl.ds(feats - edge, edge)], edge_coef.at[0], edge_send.at[4], edge_recv.at[4], after),
            remote(coef_two.at[pl.ds(0, edge)], edge_coef.at[1], edge_send.at[5], edge_recv.at[5], before),
            remote(flags.at[pl.ds(0, 8)], flags.at[pl.ds(8, 8)], edge_send.at[6], edge_recv.at[6], after),
            remote(flags.at[pl.ds(0, 8)], flags.at[pl.ds(16, 8)], edge_send.at[7], edge_recv.at[7], before),
        ]
    )
    window = sorted([d for d in range(-REACH, REACH) if d], key=lambda d: -abs(d))
    across = sorted(range(NEAR, chips, NEAR), key=lambda d: -min(d, chips - d))

    for r in range(3):
        part[...] = fitted(1 - c)
        if r == 0:
            pl.semaphore_wait(barrier, NEAR + 2)
            hello(word.at[0], same(REACH))
            hello(word.at[0], same(-REACH))
        to_partner = remote(part, sent.at[r], pair_send.at[r], pair_recv.at[r], partner)
        to_partner.start()
        mine_half = fitted(c)
        if r == 0:
            pl.semaphore_wait(word.at[0], 2)
            hello(word.at[1], same(NEAR))
            hello(word.at[1], same(-NEAR))
        to_partner.wait_recv()
        half[...] = (mine_half + sent[r]).reshape(NEAR, piece, BLOCK)
        for d in window:
            remote(half.at[lax.rem(k + d + NEAR, NEAR)], near.at[r, d + REACH], near_send.at[r], near_recv.at[r], same(d)).start()
        drain(near.at[r, pl.ds(0, NEAR - 1)], near_recv.at[r])
        acc = half[k]
        for d in range(-REACH, REACH):
            if d:
                acc = acc + near[r, d + REACH]
        own[r] = acc
        far[r, block] = acc
        if r == 0:
            pl.semaphore_wait(word.at[1], 2)
        for d in across:
            remote(own.at[r], far.at[r, block], far_send.at[r], far_recv.at[r], same(d)).start()
        if r == 0:
            edges[6].start()
            edges[7].start()
            transpose_design()
        drain(far.at[r, pl.ds(0, blocks - 1)], far_recv.at[r])
        acc = far[r, 0]
        for j in range(1, blocks):
            acc = acc + far[r, j]
        acc = acc - tgt[c, k]
        total[r] = acc
        misfit[r, c, k] = acc
        for d in window:
            remote(total.at[r], misfit.at[r, c, k], all_send.at[r], all_recv.at[r], same(d)).start()
        drain(near.at[r, pl.ds(0, NEAR - 1)], all_recv.at[r])
        forward = remote(misfit.at[r, c], misfit.at[r, c], pass_send.at[r], pass_recv.at[r], partner)
        forward.start()
        if r:
            for e in edges[:2] if r == 1 else edges[2:6]:
                e.start()
        if r == 2:
            keep = pltpu.make_async_copy(coef_two, coef_home, load_sem.at[6 + CHUNKS])
            keep.start()
        for second in range(2):
            h = 1 - c if second else c
            if second:
                forward.wait_recv()
            high, low = halves(misfit[r, h].reshape(half_rows, BLOCK))
            pair = jnp.concatenate([high, low], axis=1)
            for i in range(CHUNKS):
                here = pl.ds(i * chunk, chunk)
                product = jnp.dot(cols[h, i], pair, preferred_element_type=f32)
                product = product[:chunk] + product[chunk:]
                product = product[:, :BLOCK] + product[:, BLOCK:]
                if not second:
                    corr[here, :] = product
                    continue
                product = product + corr[here, :]
                if r == 2:
                    top = jnp.max(jnp.abs(product), axis=0, keepdims=True)
                    peak = top if i == 0 else jnp.maximum(peak, top)
                    continue
                moved = point[here, :] - product * (1.0 / lipschitz)
                fresh = jnp.maximum(moved - level, 0.0) + jnp.minimum(moved + level, 0.0)
                if r == 0:
                    set_point(i, fresh + second_push * (fresh - cur[here, :]))
                else:
                    set_point(i, fresh)
                    coef_two[here, :] = fresh
                    mass = jnp.sum(jnp.abs(fresh), axis=0, keepdims=True)
                    local_mass = mass if i == 0 else local_mass + mass
        to_partner.wait_send()
        forward.wait_send()
        drain(near.at[r, pl.ds(0, NEAR - 1)], near_send.at[r])
        drain(far.at[r, pl.ds(0, blocks - 1)], far_send.at[r])
        drain(near.at[r, pl.ds(0, NEAR - 1)], all_send.at[r])

    upper = lax.broadcasted_iota(jnp.int32, (8, BLOCK), 0) < 4
    mine[...] = jnp.where(upper, jnp.broadcast_to(peak, (8, BLOCK)), jnp.broadcast_to(local_mass, (8, BLOCK)))
    swap = remote(mine, theirs, end_send.at[0], end_recv.at[0], partner)
    swap.start()
    swap.wait()
    joined = jnp.where(upper, jnp.maximum(mine[...], theirs[...]), mine[...] + theirs[...])
    both[...] = joined
    fin[0] = joined
    middle = chips // 2 + 1

    def exchange(first, last, sign, other_first, other_last):
        count = last - first

        @pl.loop(0, count)
        def _(i):
            slot = last - 1 - i if sign > 0 else first + i
            remote(both, fin.at[slot], end_send.at[1], end_recv.at[1], same(slot)).start()

        drain(fin.at[pl.ds(first, count)], end_recv.at[1])
        drain(fin.at[pl.ds(first, count)], end_send.at[1])
        out = remote(fin.at[pl.ds(first, count)], fin.at[pl.ds(first, count)], end_send.at[2], end_recv.at[2], partner)
        out.start()
        out.wait_send()
        drain(fin.at[pl.ds(other_first, other_last - other_first)], end_recv.at[2])

    @pl.when(c == 0)
    def _():
        exchange(1, middle, 1, middle, chips)

    @pl.when(c == 1)
    def _():
        exchange(middle, chips, -1, 1, middle)

    def gather(s, carry):
        tile = fin[lax.rem(z - s + chips, chips)]
        return jnp.maximum(carry[0], tile), carry[1] + tile

    zero = jnp.zeros((8, BLOCK), f32)
    most, sums = lax.fori_loop(0, chips, gather, (zero, zero))
    scale = jnp.maximum(pen[...], most[0:1] / samples)
    norm = sums[4:5]
    ratio = pen[...] / scale
    square = zero[0:1]
    for h in range(2):
        t = tgt[h].reshape(half_rows, BLOCK)
        res = -misfit[2, h].reshape(half_rows, BLOCK)
        dual = t - ratio * res
        parts = [jnp.sum(v * v, axis=0, keepdims=True) for v in (t, dual, res)]
        tsum, dsum, rsum = parts if h == 0 else [a + b for a, b in zip((tsum, dsum, rsum), parts)]
    dual_value = (tsum - dsum) / (2.0 * samples)
    gap = rsum / (2.0 * samples) + pen[...] * norm - dual_value
    stats[0:1, :] = gap
    stats[1:2, :] = dual_value
    stats[2:3, :] = norm
    stats[3:8, :] = jnp.zeros((5, BLOCK), f32)
    for e in edges:
        e.wait()
    keep.wait()


def place_kernel(
    flags_home, design, edge_design, coef, edge_coef, stats_home,
    coef_out, design_out, gap, dual_value, mass,
    flags, stats, tiles, coefs, blank, in_sem, coef_sem, out_sem, coef_out_sem, small_sem,
):
    slots = coefs.shape[0]
    feats = coef.shape[0]
    own = feats // BLOCK
    edge = own // 4
    me = lax.axis_index("feat")
    get_flags = pltpu.make_async_copy(flags_home, flags, small_sem.at[0])
    get_flags.start()
    get_stats = pltpu.make_async_copy(stats_home, stats, small_sem.at[1])
    get_stats.start()
    blank[...] = jnp.zeros_like(blank)
    get_flags.wait()

    def columns(j):
        return pl.ds(pl.multiple_of(j * BLOCK, BLOCK), BLOCK)

    slot = jnp.int32(0)
    places = []
    for cand in range(own + 2 * edge):
        if cand < edge:
            row, index = 8, own - edge + cand
        elif cand < edge + own:
            row, index = 0, cand - edge
        else:
            row, index = 16, cand - edge - own
        arrived = jnp.logical_and(flags[row, index] == 0, flags[row + 1, index] == me)
        places.append((arrived, slot))
        slot = slot + arrived.astype(jnp.int32)

    for cand, (arrived, where) in enumerate(places):
        if edge <= cand < edge + own:
            continue
        side, j = (0, cand) if cand < edge else (1, cand - edge - own)
        bank = side * edge + j

        @pl.when(arrived)
        def _():
            pltpu.make_async_copy(edge_design.at[side, :, columns(j)], tiles.at[bank], in_sem.at[bank]).start()
            pltpu.make_async_copy(edge_coef.at[side, columns(j), :], coefs.at[cand], coef_sem.at[cand]).start()

    for cand in range(edge, edge + own):
        arrived, where = places[cand]
        j = cand - edge

        @pl.when(arrived)
        def _():
            pltpu.make_async_copy(coef.at[columns(j), :], coefs.at[cand], coef_sem.at[cand]).start()
            pltpu.make_async_copy(design.at[:, columns(j)], design_out.at[:, columns(where)], out_sem).start()

    @pl.loop(slot, slots)
    def _(s):
        pltpu.make_async_copy(blank, design_out.at[:, columns(s)], out_sem).start()
        pltpu.make_async_copy(blank.at[pl.ds(0, BLOCK)], coef_out.at[columns(s), :], coef_out_sem).start()

    get_stats.wait()
    gap[...] = stats[0:1, :]
    dual_value[...] = stats[1:2, :]
    mass[...] = stats[2:3, :]
    for cand, (arrived, where) in enumerate(places):

        @pl.when(arrived)
        def _():
            if not edge <= cand < edge + own:
                bank = cand if cand < edge else cand - own
                pltpu.make_async_copy(tiles.at[bank], tiles.at[bank], in_sem.at[bank]).wait()
                pltpu.make_async_copy(tiles.at[bank], design_out.at[:, columns(where)], out_sem).start()
            pltpu.make_async_copy(coefs.at[cand], coefs.at[cand], coef_sem.at[cand]).wait()
            pltpu.make_async_copy(coefs.at[cand], coef_out.at[columns(where), :], coef_out_sem).start()

    pltpu.make_async_copy(design_out, design_out, out_sem).wait()
    pltpu.make_async_copy(coef_out, coef_out, coef_out_sem).wait()


def local(design, targets, coef_now, coef_prev, penalty, drop_mask, dest_shard):
    samples, feats = design.shape
    devices = lax.axis_size("feat")
    chips = devices // 2
    near, blocks = NEAR, chips // NEAR
    half_rows = samples // 2
    piece = half_rows // near
    chunk = feats // CHUNKS
    edge = feats // 4
    own = feats // BLOCK
    slots = own + own // 2
    anywhere = pl.BlockSpec(memory_space=pltpu.HBM)
    vector = pl.BlockSpec(memory_space=pltpu.VMEM)
    shape = jax.ShapeDtypeStruct
    dma = pltpu.SemaphoreType.DMA

    def home(x):
        return pltpu.with_memory_space_constraint(x, pltpu.HBM)

    def mem(*dims, dtype=f32):
        return pltpu.VMEM(dims, dtype)

    coef_two, edge_design, edge_coef, flags, stats = pl.pallas_call(
        fit_kernel,
        name="fit",
        out_shape=(
            shape((feats, BLOCK), f32),
            shape((2, samples, edge), f32),
            shape((2, edge, BLOCK), f32),
            shape((24, BLOCK), jnp.int32),
            shape((8, BLOCK), f32),
        ),
        in_specs=[anywhere] * 7,
        out_specs=(anywhere, anywhere, anywhere, vector, vector),
        scratch_shapes=[
            mem(feats, BLOCK), mem(samples, feats), mem(2, near, piece, BLOCK), mem(feats, BLOCK), mem(feats, BLOCK), mem(1, BLOCK),
            mem(1, own, dtype=jnp.int32), mem(1, own, dtype=jnp.int32),
            mem(2, samples, feats, dtype=bf16), mem(2, CHUNKS, 2 * chunk, half_rows, dtype=bf16),
            mem(feats, 2 * BLOCK, dtype=bf16), mem(feats, BLOCK), mem(feats, BLOCK),
            mem(half_rows, BLOCK), mem(near, piece, BLOCK), mem(3, half_rows, BLOCK), mem(3, near, piece, BLOCK),
            mem(3, piece, BLOCK), mem(3, blocks, piece, BLOCK), mem(3, piece, BLOCK), mem(3, 2, near, piece, BLOCK),
            mem(8, BLOCK), mem(8, BLOCK), mem(8, BLOCK), mem(chips, 8, BLOCK),
            dma((7 + CHUNKS,)),
        ]
        + [dma((3,))] * 10
        + [dma((8,))] * 2
        + [dma((3,))] * 2
        + [pltpu.SemaphoreType.REGULAR((2,))],
        compiler_params=pltpu.CompilerParams(collective_id=0, has_side_effects=True, vmem_limit_bytes=56 * 2**20),
        cost_estimate=pl.CostEstimate(flops=6 * 2 * samples * feats * BLOCK, bytes_accessed=8 * 2**20, transcendentals=0),
    )(
        design,
        targets.reshape(2, near, piece, BLOCK),
        coef_now,
        coef_prev,
        penalty.reshape(1, BLOCK),
        drop_mask.reshape(1, own),
        dest_shard.reshape(1, own),
    )
    coef_out, design_out, gap, dual_value, mass = pl.pallas_call(
        place_kernel,
        name="place",
        out_shape=(
            shape((slots * BLOCK, BLOCK), f32),
            shape((samples, slots * BLOCK), f32),
            shape((1, BLOCK), f32),
            shape((1, BLOCK), f32),
            shape((1, BLOCK), f32),
        ),
        in_specs=[anywhere, vector] + [anywhere] * 4,
        out_specs=(anywhere, anywhere, vector, vector, vector),
        scratch_shapes=[
            pltpu.SMEM((24, BLOCK), jnp.int32), mem(8, BLOCK), mem(own // 2, samples, BLOCK), mem(slots, BLOCK, BLOCK), mem(samples, BLOCK),
            dma((own // 2,)), dma((slots,)), dma, dma, dma((2,)),
        ],
        compiler_params=pltpu.CompilerParams(vmem_limit_bytes=24 * 2**20),
        cost_estimate=pl.CostEstimate(flops=2**20, bytes_accessed=15 * 2**20, transcendentals=0),
    )(home(flags), design, home(edge_design), home(coef_two), home(edge_coef), home(stats))
    return (coef_out, design_out, gap.reshape(BLOCK), dual_value.reshape(BLOCK), mass.reshape(BLOCK))


def solution(mesh):
    placed = (
        P("groups", "feat"),
        P("groups", None),
        P(("groups", "feat"), None),
        P(("groups", "feat"), None),
        P("groups"),
        P(("groups", "feat")),
        P(("groups", "feat")),
    )
    return jax.shard_map(
        local,
        mesh=mesh,
        in_specs=placed,
        out_specs=(
            P(("groups", "feat"), None),
            P("groups", "feat"),
            P("groups"),
            P("groups"),
            P("groups"),
        ),
        check_vma=False,
    )
```
